32 devices in a mesh: tm: 8 (over z, y), space: 4 (over x, core).
Axes of the slice: x: 2, y: 2, z: 4, core: 2. Of those that a mesh axis runs over, the one named last changes fastest.
Arguments:
- start_values: float32 [8, 2, 1024, 1024], P('tm', None, 'space'), may hold values from -6 to 6
- node_values: float32 [8, 2, 2, 1024, 1024], P('tm', None, None, 'space'), may hold values from -6 to 6
Outputs:
- next_start: float32 [8, 2, 1024, 1024], P('tm', None, 'space')
- next_nodes: float32 [8, 2, 2, 1024, 1024], P('tm', None, None, 'space')
The draws below stay inside these ranges and needn't reach their ends.
All inputs are finite; a program needn't handle non-finite values.
Results may differ from the reference program's by a relative error of at most 0.00002.
Values sent between devices are 32-bit elements; how exact they have to be, the bound alone decides.
A program may use at most 64 MiB of HBM per device.

```python
import jax
import jax.numpy as jnp
from jax import lax

KX = 1024
KY = 1024
CX = 256
NT = 8


def block_scale(stream_key, dims, shards, low, largest):
    loudness, own = 1.0, jax.random.fold_in(stream_key, 6)
    for dim, shards_of in shards:
        heights = jnp.exp(jax.random.uniform(jax.random.fold_in(own, dim), (shards_of,), jnp.float32, low / len(shards), largest / len(shards)))
        loudness = loudness * jnp.repeat(heights, dims[dim] // shards_of).reshape([-1 if axis == dim else 1 for axis in range(len(dims))])
    return loudness


def scatter_about(key, dims, width, reach, pieces=(), held_as=jnp.bfloat16):
    factor_of = block_scale(key, dims, pieces, -0.22, 0.18) if pieces else 1.0
    values = jax.random.normal(key, dims, jnp.float32) * width * factor_of
    return jnp.minimum(jnp.maximum(values, -reach), reach).astype(held_as)


def setup_inputs(seed: int = 0) -> dict:
    key_list = jax.random.split(jax.random.key(seed), 3)
    start_values = scatter_about(key_list[0], (NT, 2, KX, KY), 1.0, 6.0, ((0, 8), (2, 4)), jnp.float32)
    node_values = scatter_about(key_list[1], (NT, 2, 2, KX, KY), 1.0, 6.0, ((0, 8), (3, 4)), jnp.float32)
    return dict(start_values=start_values, node_values=node_values)


diffusion = 1.5
drift = 0.8
shear = 0.6
first_weights = (5.0 / 24.0, 1.0 / 3.0, -1.0 / 24.0)
second_weights = (-1.0 / 24.0, 1.0 / 3.0, 5.0 / 24.0)
whole_weights = (1.0 / 6.0, 2.0 / 3.0, 1.0 / 6.0)


def spectrum(row_index, column_index):
    along = (row_index.astype(jnp.float32) - KX // 2) / (KX // 2)
    across = (column_index.astype(jnp.float32) - KY // 2) / (KY // 2)
    real_rate = -diffusion * (along[:, None] * along[:, None] + across[None, :] * across[None, :])
    imag_rate = -drift * across[None, :] + 0.0 * along[:, None]
    return real_rate, imag_rate, across


def multiply(real_rate, imag_rate, field):
    return jnp.stack([real_rate * field[..., 0, :, :] - imag_rate * field[..., 1, :, :],
                      real_rate * field[..., 1, :, :] + imag_rate * field[..., 0, :, :]], axis=-3)


def divide(real_part, imag_part, field):
    modulus = real_part * real_part + imag_part * imag_part
    return jnp.stack([(field[..., 0, :, :] * real_part + field[..., 1, :, :] * imag_part) / modulus,
                      (field[..., 1, :, :] * real_part - field[..., 0, :, :] * imag_part) / modulus], axis=-3)


def coupling_of(padded, across):
    sums = padded[..., 2:, :] + padded[..., :-2, :]
    factor = shear * across
    return jnp.stack([factor * sums[..., 1, :, :], -factor * sums[..., 0, :, :]], axis=-3)


def explicit(field, across):
    widths = [(0, 0)] * (field.ndim - 2) + [(1, 1), (0, 0)]
    return coupling_of(jnp.pad(field, widths), across)


def fine_section(begin_value, old_nodes):
    real_rate, imag_rate, across = spectrum(jnp.arange(KX), jnp.arange(KY))
    stacked = jnp.stack([begin_value, old_nodes[0], old_nodes[1]])
    old_coupling = explicit(stacked, across)
    old_slopes = multiply(real_rate, imag_rate, stacked) + old_coupling
    sum_one = first_weights[0] * old_slopes[0] + first_weights[1] * old_slopes[1] + first_weights[2] * old_slopes[2]
    sum_two = second_weights[0] * old_slopes[0] + second_weights[1] * old_slopes[1] + second_weights[2] * old_slopes[2]
    half_real = 1.0 - 0.5 * real_rate
    half_imag = -0.5 * imag_rate
    node_one = divide(half_real, half_imag, begin_value - 0.5 * multiply(real_rate, imag_rate, old_nodes[0]) + sum_one)
    one_coupling = explicit(node_one[None], across)[0]
    node_two = divide(half_real, half_imag, node_one + 0.5 * (one_coupling - old_coupling[1])
                      - 0.5 * multiply(real_rate, imag_rate, old_nodes[1]) + sum_two)
    two_coupling = explicit(node_two[None], across)[0]
    integral = (whole_weights[0] * old_slopes[0]
                + whole_weights[1] * (multiply(real_rate, imag_rate, node_one) + one_coupling)
                + whole_weights[2] * (multiply(real_rate, imag_rate, node_two) + two_coupling))
    low_row = KX // 2 - CX // 2
    low_column = KY // 2 - CX // 2
    coarse_real = real_rate[low_row:low_row + CX, low_column:low_column + CX]
    coarse_imag = imag_rate[low_row:low_row + CX, low_column:low_column + CX]
    begin_coarse = begin_value[:, low_row:low_row + CX, low_column:low_column + CX]
    end_coarse = node_two[:, low_row:low_row + CX, low_column:low_column + CX]
    tau = integral[:, low_row:low_row + CX, low_column:low_column + CX] - 0.5 * multiply(coarse_real, coarse_imag, begin_coarse + end_coarse)
    offset = 0.5 * multiply(coarse_real, coarse_imag, begin_coarse - end_coarse) + tau
    return node_one, node_two, begin_coarse, end_coarse, offset


def reference(start_values, node_values):
    node_one, node_two, begin_coarse, end_coarse, offset = lax.map(
        lambda paired: fine_section(paired[0], paired[1]), (start_values, node_values))
    real_rate, imag_rate, across = spectrum(jnp.arange(KX), jnp.arange(KY))
    low_row = KX // 2 - CX // 2
    low_column = KY // 2 - CX // 2
    coarse_real = real_rate[low_row:low_row + CX, low_column:low_column + CX]
    coarse_imag = imag_rate[low_row:low_row + CX, low_column:low_column + CX]
    step_real = 1.0 - coarse_real
    step_imag = -coarse_imag
    coarse_starts = [begin_coarse[0]]
    for slice_index in range(1, NT):
        coarse_starts.append(divide(step_real, step_imag, coarse_starts[-1] + offset[slice_index - 1]))
    begin_new = jnp.stack(coarse_starts)
    end_new = divide(step_real, step_imag, begin_new + offset)
    delta_begin = begin_new - begin_coarse
    delta_end = end_new - end_coarse
    widths = ((0, 0), (0, 0), (low_row, KX - low_row - CX), (low_column, KY - low_column - CX))
    fixed_one = node_one + jnp.pad(0.5 * (delta_begin + delta_end), widths)
    fixed_two = node_two + jnp.pad(delta_end, widths)
    next_start = jnp.concatenate([start_values[:1], fixed_two[:-1]], axis=0)
    next_nodes = jnp.stack([fixed_one, fixed_two], axis=1)
    return (next_start, next_nodes)
```

```python
import jax
import jax.numpy as jnp
from jax import lax
from jax.experimental import pallas as pl
from jax.experimental.pallas import tpu as pltpu
from jax.sharding import PartitionSpec as P

CX = 256

diffusion = 1.5
drift = 0.8
shear = 0.6
first_weights = (5.0 / 24.0, 1.0 / 3.0, -1.0 / 24.0)
second_weights = (-1.0 / 24.0, 1.0 / 3.0, 5.0 / 24.0)
whole_weights = (1.0 / 6.0, 2.0 / 3.0, 1.0 / 6.0)

MESH = pl.DeviceIdType.MESH
HALO = 8
BLOCK = 32
LANES = 128


def weighted(weights, fields):
    return [sum(w * f[k] for w, f in zip(weights, fields)) for k in range(2)]


def times(real, imag, field):
    return [real * field[0] - imag * field[1], real * field[1] + imag * field[0]]


def coupled(factor, field):
    length = field[0].shape[0]
    sums = [pltpu.roll(f, 1, 0) + pltpu.roll(f, length - 1, 0) for f in field]
    return [factor * sums[1], -factor * sums[0]]


def kernel(
    begin_hbm,
    nodes_hbm,
    start_out,
    nodes_out,
    ext,
    gain,
    shift,
    load_sem,
    start_sem,
    halo_send,
    halo_recv,
    bulk_send,
    bulk_recv,
    relay_send,
    relay_recv,
):
    slab, columns = begin_hbm.shape[1:]
    peers, count = lax.axis_size("space"), lax.axis_size("tm")
    total = slab * peers
    tm, rank = lax.axis_index("tm"), lax.axis_index("space")
    has_prev, has_next = tm > 0, tm < count - 1
    has_up, has_down = rank > 0, rank < peers - 1
    blocks = slab // BLOCK
    low_row = total // 2 - CX // 2
    low_column = columns // 2 - CX // 2
    coarse_rows = gain.shape[1]
    coarse_blocks = coarse_rows // BLOCK
    coarse_rank = (rank * slab < low_row + CX) & (rank * slab + slab > low_row)
    lower = rank < peers // 2
    coarse_start = jnp.clip(low_row - rank * slab, 0, slab - coarse_rows)
    coarse_block = coarse_start // BLOCK
    first = jnp.where(
        coarse_rank,
        jnp.where(lower, coarse_block, blocks - coarse_block - coarse_blocks),
        0,
    )

    def mirrored(index):
        return jnp.where(lower, index, blocks - 1 - index)

    def block_of(step):
        return mirrored(jnp.where(step < blocks - first, first + step, blocks - 1 - step))

    def load_of(step):
        later = jnp.where(step <= blocks - first, first + step - 1, blocks - 1 - step)
        early = jnp.where(step == 2, first - 1, first + step)
        moved = jnp.where(step <= 2, early, later)
        return mirrored(jnp.where(first == 0, step, moved))

    def rows_of(block):
        return pl.ds(pl.multiple_of(block * BLOCK, BLOCK), BLOCK)

    def loads(step):
        block = load_of(step)
        source = rows_of(block)
        target = pl.ds(pl.multiple_of(block * BLOCK + HALO, HALO), BLOCK)
        return (
            pltpu.make_async_copy(
                begin_hbm.at[:, source, :], ext.at[0, :, target, :], load_sem.at[0, step]
            ),
            pltpu.make_async_copy(
                nodes_hbm.at[:, :, source, :],
                ext.at[1:3, :, target, :],
                load_sem.at[1, step],
            ),
        )

    def halos(side):
        source = pl.ds(0 if side == 0 else slab - HALO, HALO)
        target = pl.ds(slab + HALO if side == 0 else 0, HALO)
        there = {"space": rank - 1 if side == 0 else rank + 1}
        return (
            pltpu.make_async_remote_copy(
                begin_hbm.at[:, source, :],
                ext.at[0, :, target, :],
                halo_send.at[0, side],
                halo_recv.at[0, side],
                device_id=there,
                device_id_type=MESH,
            ),
            pltpu.make_async_remote_copy(
                nodes_hbm.at[:, :, source, :],
                ext.at[1:3, :, target, :],
                halo_send.at[1, side],
                halo_recv.at[1, side],
                device_id=there,
                device_id_type=MESH,
            ),
        )

    following = {"tm": tm + 1}

    def relay_copy(step):
        place = (slice(None), rows_of(block_of(step)), pl.ds(low_column, CX))
        return pltpu.make_async_remote_copy(
            nodes_out.at[(1,) + place],
            start_out.at[place],
            relay_send.at[step],
            relay_recv.at[step],
            device_id=following,
            device_id_type=MESH,
        )

    def bulk(unit, act):
        step, half = unit // 2, unit % 2
        rows = rows_of(block_of(step))
        strip = coarse_rank & (step < coarse_blocks)

        def copy(place):
            return pltpu.make_async_remote_copy(
                nodes_out.at[(1,) + place],
                start_out.at[place],
                bulk_send.at[unit],
                bulk_recv.at[unit],
                device_id=following,
                device_id_type=MESH,
            )

        @pl.when(strip)
        def _():
            left = pl.multiple_of(half * (low_column + CX), LANES)
            act(copy((slice(None), rows, pl.ds(left, low_column))))

        @pl.when(jnp.logical_not(strip))
        def _():
            act(copy((half, rows, slice(None))))

    def send(low, high):
        @pl.when(has_next)
        def _():
            @pl.loop(low, high)
            def _(unit):
                bulk(unit, lambda c: c.start())

    whole_start = pltpu.make_async_copy(begin_hbm, start_out, start_sem)

    @pl.loop(0, blocks)
    def _(step):
        for c in loads(step):
            c.start()

    barrier = pltpu.get_barrier_semaphore()
    for there, exists in (
        ({"space": rank - 1}, has_up),
        ({"space": rank + 1}, has_down),
        ({"tm": tm - 1}, has_prev),
        ({"tm": tm + 1}, has_next),
    ):

        @pl.when(exists)
        def _(there=there):
            pl.semaphore_signal(barrier, inc=1, device_id=there, device_id_type=MESH)

    friends = sum(jnp.where(e, 1, 0) for e in (has_up, has_down, has_prev, has_next))
    pl.semaphore_wait(barrier, friends)

    for side, exists in ((0, has_up), (1, has_down)):

        @pl.when(exists)
        def _(side=side):
            for c in halos(side):
                c.start()

        @pl.when(jnp.logical_not(exists))
        def _(side=side):
            edge = pl.ds(0 if side == 0 else slab + HALO, HALO)
            ext[:, :, edge, :] = jnp.zeros((3, 2, HALO, columns), jnp.float32)

    @pl.when(jnp.logical_not(has_prev))
    def _():
        whole_start.start()

    def strip_compute(block, column, coarse):
        length = BLOCK + 2 * HALO
        span = pl.ds(pl.multiple_of(block * BLOCK, BLOCK), length)
        here = pl.ds(column, LANES)
        begin, one, two = [[ext[f, k, span, here] for k in range(2)] for f in range(3)]
        row = lax.broadcasted_iota(jnp.int32, (length, LANES), 0)
        row = row + (rank * slab + block * BLOCK - HALO)
        along = (row - total // 2).astype(jnp.float32) / (total // 2)
        place = lax.broadcasted_iota(jnp.int32, (1, LANES), 1) + column
        across = (place - columns // 2).astype(jnp.float32) / (columns // 2)
        inside = jnp.where((row >= 0) & (row < total), 1.0, 0.0).astype(jnp.float32)
        real = -diffusion * (along * along + across * across)
        imag = -drift * across
        factor = shear * across
        half_real, half_imag = 1.0 - 0.5 * real, -0.5 * imag
        scale = 1.0 / (half_real * half_real + half_imag * half_imag)
        inverse = (half_real * scale, -half_imag * scale)
        sum_one = weighted(first_weights, (begin, one, two))
        sum_two = weighted(second_weights, (begin, one, two))
        moved = times(real, imag, [s - 0.5 * o for s, o in zip(sum_one, one)])
        turned = coupled(factor, sum_one)
        inner = [begin[k] + moved[k] + turned[k] for k in range(2)]
        node_one = [inside * f for f in times(*inverse, inner)]
        moved = times(real, imag, [s - 0.5 * o for s, o in zip(sum_two, two)])
        turned = coupled(
            factor, [sum_two[k] + 0.5 * (node_one[k] - one[k]) for k in range(2)]
        )
        inner = [node_one[k] + moved[k] + turned[k] for k in range(2)]
        node_two = times(*inverse, inner)
        own = slice(HALO, HALO + BLOCK)
        rows = rows_of(block)
        if not coarse:
            for k in range(2):
                nodes_out[0, k, rows, here] = node_one[k][own]
                nodes_out[1, k, rows, here] = node_two[k][own]
            return
        mean = weighted(whole_weights, (begin, node_one, node_two))
        moved = times(real, imag, [mean[k] - node_two[k] for k in range(2)])
        turned = coupled(factor, mean)
        offset = [moved[k] + turned[k] for k in range(2)]
        step_real, step_imag = 1.0 - real, -imag
        scale = 1.0 / (step_real * step_real + step_imag * step_imag)
        grown = (step_real * scale, -step_imag * scale)
        offset = times(*grown, offset)
        local = pl.ds(pl.multiple_of(block * BLOCK - coarse_start, BLOCK), BLOCK)
        inner_here = pl.ds(pl.multiple_of(column - low_column, LANES), LANES)
        for k in range(2):
            gain[k, local, inner_here] = grown[k][own]
            shift[k, local, inner_here] = offset[k][own]
            kept = node_one[k] - 0.5 * (begin[k] + node_two[k])
            nodes_out[0, k, rows, here] = kept[own]

    def compute(step):
        block = block_of(step)
        arrived = jnp.where(step == 0, 0, step + 2)

        @pl.loop(arrived, jnp.minimum(step + 3, blocks))
        def _(which):
            for c in loads(which):
                c.wait()

        @pl.when((block == blocks - 1) & has_down)
        def _():
            for c in halos(0):
                c.wait_recv()

        @pl.when((block == 0) & has_up)
        def _():
            for c in halos(1):
                c.wait_recv()

        in_coarse = coarse_rank & (step < coarse_blocks)

        @pl.loop(0, columns // LANES)
        def _(index):
            column = pl.multiple_of(index * LANES, LANES)
            low = index * LANES
            coarse = in_coarse & (low >= low_column) & (low < low_column + CX)

            @pl.when(coarse)
            def _():
                strip_compute(block, column, True)

            @pl.when(jnp.logical_not(coarse))
            def _():
                strip_compute(block, column, False)

    def relay():
        @pl.when(jnp.logical_not(has_prev))
        def _():
            whole_start.wait()

        @pl.loop(0, coarse_blocks)
        def _(step):
            @pl.when(has_prev)
            def _():
                relay_copy(step).wait_recv()

            block = block_of(step)
            rows = rows_of(block)
            local = pl.ds(pl.multiple_of(block * BLOCK - coarse_start, BLOCK), BLOCK)
            here = pl.ds(low_column, CX)
            begin = [start_out[k, rows, here] for k in range(2)]
            grown = times(gain[0, local, :], gain[1, local, :], begin)
            finish = [grown[k] + shift[k, local, :] for k in range(2)]
            for k in range(2):
                nodes_out[1, k, rows, here] = finish[k]

            @pl.when(has_next)
            def _():
                relay_copy(step).start()

            for k in range(2):
                nodes_out[0, k, rows, here] += 0.5 * (begin[k] + finish[k])

    units = 2 * blocks
    waiting = jnp.minimum((3 * tm) // 2, units)
    opening = jnp.where(has_prev, jnp.minimum(waiting, 2 * coarse_blocks), 2 * coarse_blocks)
    middle = jnp.maximum(waiting, opening)

    @pl.when(coarse_rank)
    def _():
        @pl.loop(0, coarse_blocks)
        def _(step):
            compute(step)

        @pl.when(jnp.logical_not(has_prev))
        def _():
            relay()

        send(0, opening)

        @pl.loop(coarse_blocks, blocks)
        def _(step):
            compute(step)

        send(opening, middle)

        @pl.when(has_prev)
        def _():
            relay()

        send(middle, units)

    @pl.when(jnp.logical_not(coarse_rank))
    def _():
        @pl.loop(0, blocks)
        def _(step):
            compute(step)
            send(2 * step, 2 * step + 2)

        @pl.when(jnp.logical_not(has_prev))
        def _():
            whole_start.wait()

    for side, exists in ((0, has_up), (1, has_down)):

        @pl.when(exists)
        def _(side=side):
            for c in halos(side):
                c.wait_send()

    @pl.when(coarse_rank & has_next)
    def _():
        @pl.loop(0, coarse_blocks)
        def _(step):
            relay_copy(step).wait_send()

    @pl.when(has_prev)
    def _():
        @pl.loop(0, units)
        def _(unit):
            bulk(unit, lambda c: c.wait_recv())

    @pl.when(has_next)
    def _():
        @pl.loop(0, units)
        def _(unit):
            bulk(unit, lambda c: c.wait_send())


def body(start_values, node_values):
    slab, columns = start_values.shape[2:]
    peers = lax.axis_size("space")
    coarse_rows = min(slab, max(CX // 2, CX // peers))
    blocks, coarse_blocks = slab // BLOCK, coarse_rows // BLOCK
    hbm = pl.BlockSpec(memory_space=pltpu.HBM)
    vmem = pl.BlockSpec(memory_space=pltpu.VMEM)
    dma = pltpu.SemaphoreType.DMA
    start, nodes = pl.pallas_call(
        kernel,
        out_shape=(
            OUT((2, slab, columns), jnp.float32),
            OUT((2, 2, slab, columns), jnp.float32),
        ),
        in_specs=[hbm, hbm],
        out_specs=(vmem, vmem),
        scratch_shapes=[
            pltpu.VMEM((3, 2, slab + 2 * HALO, columns), jnp.float32),
            pltpu.VMEM((2, coarse_rows, CX), jnp.float32),
            pltpu.VMEM((2, coarse_rows, CX), jnp.float32),
            dma((2, blocks)),
            dma,
            dma((2, 2)),
            dma((2, 2)),
            dma((2 * blocks,)),
            dma((2 * blocks,)),
            dma((coarse_blocks,)),
            dma((coarse_blocks,)),
        ],
        compiler_params=pltpu.CompilerParams(
            collective_id=0, has_side_effects=True, vmem_limit_bytes=56 * 1024 * 1024
        ),
    )(start_values[0], node_values[0])
    return (start[None], nodes[None])


OUT = pltpu.VMEM


def solution(mesh):
    in_specs = (P("tm", None, "space", None), P("tm", None, None, "space", None))
    out_specs = (P("tm", None, "space", None), P("tm", None, None, "space", None))
    return jax.shard_map(body, mesh=mesh, in_specs=in_specs, out_specs=out_specs, check_vma=False)
```

```python
import jax
import jax.numpy as jnp
from jax import lax
from jax.experimental import pallas as pl
from jax.experimental.pallas import tpu as pltpu
from jax.sharding import PartitionSpec as P

CX = 256

diffusion = 1.5
drift = 0.8
shear = 0.6
first_weights = (5.0 / 24.0, 1.0 / 3.0, -1.0 / 24.0)
second_weights = (-1.0 / 24.0, 1.0 / 3.0, 5.0 / 24.0)
whole_weights = (1.0 / 6.0, 2.0 / 3.0, 1.0 / 6.0)

MESH = pl.DeviceIdType.MESH
HALO = 8
BLOCK = 32
PARTS = 4
LANES = 128


def weighted(weights, fields):
    return [sum(w * f[k] for w, f in zip(weights, fields)) for k in range(2)]


def times(real, imag, field):
    return [real * field[0] - imag * field[1], real * field[1] + imag * field[0]]


def coupled(factor, field):
    length = field[0].shape[0]
    sums = [pltpu.roll(f, 1, 0) + pltpu.roll(f, length - 1, 0) for f in field]
    return [factor * sums[1], -factor * sums[0]]


def kernel(
    begin_hbm,
    nodes_hbm,
    start_out,
    nodes_out,
    ext,
    gain,
    shift,
    load_sem,
    start_sem,
    halo_send,
    halo_recv,
    bulk_send,
    bulk_recv,
    relay_send,
    relay_recv,
):
    slab, columns = begin_hbm.shape[1:]
    peers, count = lax.axis_size("space"), lax.axis_size("tm")
    total = slab * peers
    tm, rank = lax.axis_index("tm"), lax.axis_index("space")
    has_prev, has_next = tm > 0, tm < count - 1
    has_up, has_down = rank > 0, rank < peers - 1
    blocks = slab // BLOCK
    low_row = total // 2 - CX // 2
    low_column = columns // 2 - CX // 2
    coarse_rows = gain.shape[1]
    coarse_blocks = coarse_rows // BLOCK
    coarse_rank = (rank * slab < low_row + CX) & (rank * slab + slab > low_row)
    lower = rank < peers // 2
    coarse_start = jnp.clip(low_row - rank * slab, 0, slab - coarse_rows)
    coarse_block = coarse_start // BLOCK
    first = jnp.where(
        coarse_rank,
        jnp.where(lower, coarse_block, blocks - coarse_block - coarse_blocks),
        0,
    )

    def mirrored(index):
        return jnp.where(lower, index, blocks - 1 - index)

    def block_of(step):
        return mirrored(jnp.where(step < blocks - first, first + step, blocks - 1 - step))

    def load_of(step):
        later = jnp.where(step <= blocks - first, first + step - 1, blocks - 1 - step)
        early = jnp.where(step == 2, first - 1, first + step)
        moved = jnp.where(step <= 2, early, later)
        return mirrored(jnp.where(first == 0, step, moved))

    def rows_of(block):
        return pl.ds(pl.multiple_of(block * BLOCK, BLOCK), BLOCK)

    def loads(step):
        block = load_of(step)
        source = rows_of(block)
        target = pl.ds(pl.multiple_of(block * BLOCK + HALO, HALO), BLOCK)
        return (
            pltpu.make_async_copy(
                begin_hbm.at[:, source, :], ext.at[0, :, target, :], load_sem.at[0, step]
            ),
            pltpu.make_async_copy(
                nodes_hbm.at[:, :, source, :],
                ext.at[1:3, :, target, :],
                load_sem.at[1, step],
            ),
        )

    def halos(side):
        source = pl.ds(0 if side == 0 else slab - HALO, HALO)
        target = pl.ds(slab + HALO if side == 0 else 0, HALO)
        there = {"space": rank - 1 if side == 0 else rank + 1}
        return (
            pltpu.make_async_remote_copy(
                begin_hbm.at[:, source, :],
                ext.at[0, :, target, :],
                halo_send.at[0, side],
                halo_recv.at[0, side],
                device_id=there,
                device_id_type=MESH,
            ),
            pltpu.make_async_remote_copy(
                nodes_hbm.at[:, :, source, :],
                ext.at[1:3, :, target, :],
                halo_send.at[1, side],
                halo_recv.at[1, side],
                device_id=there,
                device_id_type=MESH,
            ),
        )

    following = {"tm": tm + 1}

    def relay_copy(step):
        place = (slice(None), rows_of(block_of(step)), pl.ds(low_column, CX))
        return pltpu.make_async_remote_copy(
            nodes_out.at[(1,) + place],
            start_out.at[place],
            relay_send.at[step],
            relay_recv.at[step],
            device_id=following,
            device_id_type=MESH,
        )

    def bulk(unit, act):
        step, part = unit // PARTS, unit % PARTS
        block = block_of(step)
        strip = coarse_rank & (step < coarse_blocks)

        def copy(place):
            return pltpu.make_async_remote_copy(
                nodes_out.at[(1,) + place],
                start_out.at[place],
                bulk_send.at[unit],
                bulk_recv.at[unit],
                device_id=following,
                device_id_type=MESH,
            )

        @pl.when(strip)
        def _():
            height = 2 * BLOCK // PARTS
            top = pl.multiple_of(block * BLOCK + (part // 2) * height, HALO)
            left = pl.multiple_of((part % 2) * (low_column + CX), LANES)
            act(copy((slice(None), pl.ds(top, height), pl.ds(left, low_column))))

        @pl.when(jnp.logical_not(strip))
        def _():
            width = columns // PARTS
            left = pl.multiple_of(part * width, LANES)
            act(copy((slice(None), rows_of(block), pl.ds(left, width))))

    def send(low, high):
        @pl.when(has_next)
        def _():
            @pl.loop(low, high)
            def _(unit):
                bulk(unit, lambda c: c.start())

    whole_start = pltpu.make_async_copy(begin_hbm, start_out, start_sem)

    barrier = pltpu.get_barrier_semaphore()
    for there, exists in (
        ({"space": rank - 1}, has_up),
        ({"space": rank + 1}, has_down),
        ({"tm": tm - 1}, has_prev),
        ({"tm": tm + 1}, has_next),
    ):

        @pl.when(exists)
        def _(there=there):
            pl.semaphore_signal(barrier, inc=1, device_id=there, device_id_type=MESH)

    @pl.loop(0, blocks)
    def _(step):
        for c in loads(step):
            c.start()

    for side, exists in ((0, has_up), (1, has_down)):

        @pl.when(jnp.logical_not(exists))
        def _(side=side):
            edge = pl.ds(0 if side == 0 else slab + HALO, HALO)
            ext[:, :, edge, :] = jnp.zeros((3, 2, HALO, columns), jnp.float32)

    @pl.when(jnp.logical_not(has_prev))
    def _():
        whole_start.start()

    def greet():
        friends = sum(jnp.where(e, 1, 0) for e in (has_up, has_down, has_prev, has_next))
        pl.semaphore_wait(barrier, friends)
        for side, exists in ((0, has_up), (1, has_down)):

            @pl.when(exists)
            def _(side=side):
                for c in halos(side):
                    c.start()

    def strip_compute(block, column, coarse):
        length = BLOCK + 2 * HALO
        span = pl.ds(pl.multiple_of(block * BLOCK, BLOCK), length)
        here = pl.ds(column, LANES)
        begin, one, two = [[ext[f, k, span, here] for k in range(2)] for f in range(3)]
        row = lax.broadcasted_iota(jnp.int32, (length, LANES), 0)
        row = row + (rank * slab + block * BLOCK - HALO)
        along = (row - total // 2).astype(jnp.float32) / (total // 2)
        place = lax.broadcasted_iota(jnp.int32, (1, LANES), 1) + column
        across = (place - columns // 2).astype(jnp.float32) / (columns // 2)
        inside = jnp.where((row >= 0) & (row < total), 1.0, 0.0).astype(jnp.float32)
        real = -diffusion * (along * along + across * across)
        imag = -drift * across
        factor = shear * across
        half_real, half_imag = 1.0 - 0.5 * real, -0.5 * imag
        scale = 1.0 / (half_real * half_real + half_imag * half_imag)
        inverse = (half_real * scale, -half_imag * scale)
        sum_one = weighted(first_weights, (begin, one, two))
        sum_two = weighted(second_weights, (begin, one, two))
        moved = times(real, imag, [s - 0.5 * o for s, o in zip(sum_one, one)])
        turned = coupled(factor, sum_one)
        inner = [begin[k] + moved[k] + turned[k] for k in range(2)]
        node_one = [inside * f for f in times(*inverse, inner)]
        moved = times(real, imag, [s - 0.5 * o for s, o in zip(sum_two, two)])
        turned = coupled(
            factor, [sum_two[k] + 0.5 * (node_one[k] - one[k]) for k in range(2)]
        )
        inner = [node_one[k] + moved[k] + turned[k] for k in range(2)]
        node_two = times(*inverse, inner)
        own = slice(HALO, HALO + BLOCK)
        rows = rows_of(block)
        if not coarse:
            for k in range(2):
                nodes_out[0, k, rows, here] = node_one[k][own]
                nodes_out[1, k, rows, here] = node_two[k][own]
            return
        mean = weighted(whole_weights, (begin, node_one, node_two))
        moved = times(real, imag, [mean[k] - node_two[k] for k in range(2)])
        turned = coupled(factor, mean)
        offset = [moved[k] + turned[k] for k in range(2)]
        step_real, step_imag = 1.0 - real, -imag
        scale = 1.0 / (step_real * step_real + step_imag * step_imag)
        grown = (step_real * scale, -step_imag * scale)
        offset = times(*grown, offset)
        local = pl.ds(pl.multiple_of(block * BLOCK - coarse_start, BLOCK), BLOCK)
        inner_here = pl.ds(pl.multiple_of(column - low_column, LANES), LANES)
        for k in range(2):
            gain[k, local, inner_here] = grown[k][own]
            shift[k, local, inner_here] = offset[k][own]
            kept = node_one[k] - 0.5 * (begin[k] + node_two[k])
            nodes_out[0, k, rows, here] = kept[own]

    lead = jnp.where(first == 0, 2, 3)

    def compute(step, after=None):
        block = block_of(step)
        arrived = jnp.where(step == 0, 0, step + lead - 1)

        @pl.loop(arrived, jnp.minimum(step + lead, blocks))
        def _(which):
            for c in loads(which):
                c.wait()

        @pl.when((block == blocks - 1) & has_down)
        def _():
            for c in halos(0):
                c.wait_recv()

        @pl.when((block == 0) & has_up)
        def _():
            for c in halos(1):
                c.wait_recv()

        in_coarse = coarse_rank & (step < coarse_blocks)
        strips = columns // LANES // PARTS

        @pl.loop(0, PARTS)
        def _(part):
            @pl.loop(0, strips)
            def _(index):
                low = (part * strips + index) * LANES
                column = pl.multiple_of(low, LANES)
                if after is not None:
                    strip_compute(block, column, False)
                    return
                coarse = in_coarse & (low >= low_column) & (low < low_column + CX)

                @pl.when(coarse)
                def _():
                    strip_compute(block, column, True)

                @pl.when(jnp.logical_not(coarse))
                def _():
                    strip_compute(block, column, False)

            if after is not None:
                after(PARTS * step + part)

    def relay():
        @pl.when(jnp.logical_not(has_prev))
        def _():
            whole_start.wait()

        @pl.loop(0, coarse_blocks)
        def _(step):
            @pl.when(has_prev)
            def _():
                relay_copy(step).wait_recv()

            block = block_of(step)
            rows = rows_of(block)
            local = pl.ds(pl.multiple_of(block * BLOCK - coarse_start, BLOCK), BLOCK)
            here = pl.ds(low_column, CX)
            begin = [start_out[k, rows, here] for k in range(2)]
            grown = times(gain[0, local, :], gain[1, local, :], begin)
            finish = [grown[k] + shift[k, local, :] for k in range(2)]
            for k in range(2):
                nodes_out[1, k, rows, here] = finish[k]

            @pl.when(has_next)
            def _():
                relay_copy(step).start()

            for k in range(2):
                nodes_out[0, k, rows, here] += 0.5 * (begin[k] + finish[k])

    units = PARTS * blocks
    waiting = jnp.minimum((3 * PARTS * tm) // 4, units)
    opening = jnp.where(has_prev, jnp.minimum(waiting, PARTS * coarse_blocks), PARTS * coarse_blocks)
    middle = jnp.maximum(waiting, opening)

    @pl.when(coarse_rank)
    def _():
        greet()

        @pl.loop(0, coarse_blocks)
        def _(step):
            compute(step)

        @pl.when(jnp.logical_not(has_prev))
        def _():
            relay()

        send(0, opening)

        @pl.loop(coarse_blocks, blocks)
        def _(step):
            compute(step)

        send(opening, middle)

        @pl.when(has_prev)
        def _():
            relay()

        send(middle, units)

    @pl.when(jnp.logical_not(coarse_rank))
    def _():
        def after(unit):
            @pl.when(unit == 0)
            def _():
                greet()

            send(unit, unit + 1)

        @pl.loop(0, blocks)
        def _(step):
            compute(step, after)

        @pl.when(jnp.logical_not(has_prev))
        def _():
            whole_start.wait()

    for side, exists in ((0, has_up), (1, has_down)):

        @pl.when(exists)
        def _(side=side):
            for c in halos(side):
                c.wait_send()

    @pl.when(coarse_rank & has_next)
    def _():
        @pl.loop(0, coarse_blocks)
        def _(step):
            relay_copy(step).wait_send()

    @pl.when(has_prev)
    def _():
        @pl.loop(0, units)
        def _(unit):
            bulk(unit, lambda c: c.wait_recv())

    @pl.when(has_next)
    def _():
        @pl.loop(0, units)
        def _(unit):
            bulk(unit, lambda c: c.wait_send())


def write_out(start, nodes, start_hbm, nodes_hbm, sem):
    copies = [
        pltpu.make_async_copy(nodes.at[f, k], nodes_hbm.at[f, k], sem.at[2 * f + k])
        for f in range(2)
        for k in range(2)
    ]
    copies += [pltpu.make_async_copy(start.at[k], start_hbm.at[k], sem.at[4 + k]) for k in range(2)]
    for c in copies:
        c.start()
    for c in copies:
        c.wait()


def body(start_values, node_values):
    slab, columns = start_values.shape[2:]
    peers = lax.axis_size("space")
    coarse_rows = min(slab, max(CX // 2, CX // peers))
    blocks, coarse_blocks = slab // BLOCK, coarse_rows // BLOCK
    hbm = pl.BlockSpec(memory_space=pltpu.HBM)
    vmem = pl.BlockSpec(memory_space=pltpu.VMEM)
    dma = pltpu.SemaphoreType.DMA
    start, nodes = pl.pallas_call(
        kernel,
        out_shape=(
            OUT((2, slab, columns), jnp.float32),
            OUT((2, 2, slab, columns), jnp.float32),
        ),
        in_specs=[hbm, hbm],
        out_specs=(vmem, vmem),
        scratch_shapes=[
            pltpu.VMEM((3, 2, slab + 2 * HALO, columns), jnp.float32),
            pltpu.VMEM((2, coarse_rows, CX), jnp.float32),
            pltpu.VMEM((2, coarse_rows, CX), jnp.float32),
            dma((2, blocks)),
            dma,
            dma((2, 2)),
            dma((2, 2)),
            dma((PARTS * blocks,)),
            dma((PARTS * blocks,)),
            dma((coarse_blocks,)),
            dma((coarse_blocks,)),
        ],
        compiler_params=pltpu.CompilerParams(
            collective_id=0, has_side_effects=True, vmem_limit_bytes=56 * 1024 * 1024
        ),
    )(start_values[0], node_values[0])
    start, nodes = pl.pallas_call(
        write_out,
        out_shape=(
            jax.ShapeDtypeStruct(start.shape, jnp.float32),
            jax.ShapeDtypeStruct(nodes.shape, jnp.float32),
        ),
        in_specs=[pl.BlockSpec(memory_space=pl.ANY)] * 2,
        out_specs=(hbm, hbm),
        scratch_shapes=[dma((6,))],
        compiler_params=pltpu.CompilerParams(vmem_limit_bytes=2 * 1024 * 1024),
    )(start, nodes)
    return (start[None], nodes[None])


OUT = pltpu.VMEM


def solution(mesh):
    in_specs = (P("tm", None, "space", None), P("tm", None, None, "space", None))
    out_specs = (P("tm", None, "space", None), P("tm", None, None, "space", None))
    return jax.shard_map(body, mesh=mesh, in_specs=in_specs, out_specs=out_specs, check_vma=False)
```

```python
import jax
import jax.numpy as jnp
from jax import lax
from jax.experimental import pallas as pl
from jax.experimental.pallas import tpu as pltpu
from jax.sharding import PartitionSpec as P

CX = 256

diffusion = 1.5
drift = 0.8
shear = 0.6
first_weights = (5.0 / 24.0, 1.0 / 3.0, -1.0 / 24.0)
second_weights = (-1.0 / 24.0, 1.0 / 3.0, 5.0 / 24.0)
whole_weights = (1.0 / 6.0, 2.0 / 3.0, 1.0 / 6.0)

MESH = pl.DeviceIdType.MESH
HALO = 8
BLOCK = 32
PARTS = 4
STRIPS = 2
WHOLES = 1
LANES = 128


def weighted(weights, fields):
    return [sum(w * f[k] for w, f in zip(weights, fields)) for k in range(2)]


def times(real, imag, field):
    return [real * field[0] - imag * field[1], real * field[1] + imag * field[0]]


def coupled(factor, field):
    length = field[0].shape[0]
    sums = [pltpu.roll(f, 1, 0) + pltpu.roll(f, length - 1, 0) for f in field]
    return [factor * sums[1], -factor * sums[0]]


def kernel(
    begin_hbm,
    nodes_hbm,
    start_out,
    nodes_out,
    ext,
    gain,
    shift,
    load_sem,
    start_sem,
    halo_send,
    halo_recv,
    bulk_send,
    bulk_recv,
    relay_send,
    relay_recv,
):
    slab, columns = begin_hbm.shape[1:]
    peers, count = lax.axis_size("space"), lax.axis_size("tm")
    total = slab * peers
    tm, rank = lax.axis_index("tm"), lax.axis_index("space")
    has_prev, has_next = tm > 0, tm < count - 1
    has_up, has_down = rank > 0, rank < peers - 1
    blocks = slab // BLOCK
    low_row = total // 2 - CX // 2
    low_column = columns // 2 - CX // 2
    coarse_rows = gain.shape[1]
    coarse_blocks = coarse_rows // BLOCK
    coarse_rank = (rank * slab < low_row + CX) & (rank * slab + slab > low_row)
    lower = rank < peers // 2
    coarse_start = jnp.clip(low_row - rank * slab, 0, slab - coarse_rows)
    coarse_block = coarse_start // BLOCK
    first = jnp.where(
        coarse_rank,
        jnp.where(lower, coarse_block, blocks - coarse_block - coarse_blocks),
        0,
    )

    def mirrored(index):
        return jnp.where(lower, index, blocks - 1 - index)

    def block_of(step):
        return mirrored(jnp.where(step < blocks - first, first + step, blocks - 1 - step))

    def load_of(step):
        later = jnp.where(step <= blocks - first, first + step - 1, blocks - 1 - step)
        early = jnp.where(step == 2, first - 1, first + step)
        moved = jnp.where(step <= 2, early, later)
        return mirrored(jnp.where(first == 0, step, moved))

    def rows_of(block):
        return pl.ds(pl.multiple_of(block * BLOCK, BLOCK), BLOCK)

    def loads(step):
        block = load_of(step)
        source = rows_of(block)
        target = pl.ds(pl.multiple_of(block * BLOCK + HALO, HALO), BLOCK)
        return (
            pltpu.make_async_copy(
                begin_hbm.at[:, source, :], ext.at[0, :, target, :], load_sem.at[0, step]
            ),
            pltpu.make_async_copy(
                nodes_hbm.at[:, :, source, :],
                ext.at[1:3, :, target, :],
                load_sem.at[1, step],
            ),
        )

    def halos(side):
        source = pl.ds(0 if side == 0 else slab - HALO, HALO)
        target = pl.ds(slab + HALO if side == 0 else 0, HALO)
        there = {"space": rank - 1 if side == 0 else rank + 1}
        return (
            pltpu.make_async_remote_copy(
                begin_hbm.at[:, source, :],
                ext.at[0, :, target, :],
                halo_send.at[0, side],
                halo_recv.at[0, side],
                device_id=there,
                device_id_type=MESH,
            ),
            pltpu.make_async_remote_copy(
                nodes_hbm.at[:, :, source, :],
                ext.at[1:3, :, target, :],
                halo_send.at[1, side],
                halo_recv.at[1, side],
                device_id=there,
                device_id_type=MESH,
            ),
        )

    following = {"tm": tm + 1}

    def relay_copy(step):
        place = (slice(None), rows_of(block_of(step)), pl.ds(low_column, CX))
        return pltpu.make_async_remote_copy(
            nodes_out.at[(1,) + place],
            start_out.at[place],
            relay_send.at[step],
            relay_recv.at[step],
            device_id=following,
            device_id_type=MESH,
        )

    def bulk(unit, act):
        step, part = unit // PARTS, unit % PARTS
        block = block_of(step)
        strip = coarse_rank & (step < coarse_blocks)

        def copy(place):
            return pltpu.make_async_remote_copy(
                nodes_out.at[(1,) + place],
                start_out.at[place],
                bulk_send.at[unit],
                bulk_recv.at[unit],
                device_id=following,
                device_id_type=MESH,
            )

        @pl.when(strip & (part >= PARTS - STRIPS))
        def _():
            height = 2 * BLOCK // STRIPS
            top = pl.multiple_of(block * BLOCK + (part - (PARTS - STRIPS)) // 2 * height, HALO)
            left = pl.multiple_of((part % 2) * (low_column + CX), LANES)
            act(copy((slice(None), pl.ds(top, height), pl.ds(left, low_column))))

        quick = (step == 0) & jnp.logical_not(coarse_rank)

        @pl.when(quick)
        def _():
            width = columns // PARTS
            left = pl.multiple_of(part * width, LANES)
            act(copy((slice(None), rows_of(block), pl.ds(left, width))))

        @pl.when(jnp.logical_not(quick | strip) & ((part + 1) % (PARTS // WHOLES) == 0))
        def _():
            width = columns // WHOLES
            left = pl.multiple_of(part // (PARTS // WHOLES) * width, LANES)
            act(copy((slice(None), rows_of(block), pl.ds(left, width))))

    def send(low, high):
        @pl.when(has_next)
        def _():
            @pl.loop(low, high)
            def _(unit):
                bulk(unit, lambda c: c.start())

    whole_start = pltpu.make_async_copy(begin_hbm, start_out, start_sem)

    barrier = pltpu.get_barrier_semaphore()
    for there, exists in (
        ({"space": rank - 1}, has_up),
        ({"space": rank + 1}, has_down),
        ({"tm": tm - 1}, has_prev),
        ({"tm": tm + 1}, has_next),
    ):

        @pl.when(exists)
        def _(there=there):
            pl.semaphore_signal(barrier, inc=1, device_id=there, device_id_type=MESH)

    @pl.loop(0, blocks)
    def _(step):
        for c in loads(step):
            c.start()

    for side, exists in ((0, has_up), (1, has_down)):

        @pl.when(jnp.logical_not(exists))
        def _(side=side):
            edge = pl.ds(0 if side == 0 else slab + HALO, HALO)
            ext[:, :, edge, :] = jnp.zeros((3, 2, HALO, columns), jnp.float32)

    @pl.when(jnp.logical_not(has_prev))
    def _():
        whole_start.start()

    def greet():
        friends = sum(jnp.where(e, 1, 0) for e in (has_up, has_down, has_prev, has_next))
        pl.semaphore_wait(barrier, friends)
        for side, exists in ((0, has_up), (1, has_down)):

            @pl.when(exists)
            def _(side=side):
                for c in halos(side):
                    c.start()

    def strip_compute(block, column, coarse):
        length = BLOCK + 2 * HALO
        span = pl.ds(pl.multiple_of(block * BLOCK, BLOCK), length)
        here = pl.ds(column, LANES)
        begin, one, two = [[ext[f, k, span, here] for k in range(2)] for f in range(3)]
        row = lax.broadcasted_iota(jnp.int32, (length, LANES), 0)
        row = row + (rank * slab + block * BLOCK - HALO)
        along = (row - total // 2).astype(jnp.float32) / (total // 2)
        place = lax.broadcasted_iota(jnp.int32, (1, LANES), 1) + column
        across = (place - columns // 2).astype(jnp.float32) / (columns // 2)
        inside = jnp.where((row >= 0) & (row < total), 1.0, 0.0).astype(jnp.float32)
        real = -diffusion * (along * along + across * across)
        imag = -drift * across
        factor = shear * across
        half_real, half_imag = 1.0 - 0.5 * real, -0.5 * imag
        scale = 1.0 / (half_real * half_real + half_imag * half_imag)
        inverse = (half_real * scale, -half_imag * scale)
        sum_one = weighted(first_weights, (begin, one, two))
        sum_two = weighted(second_weights, (begin, one, two))
        moved = times(real, imag, [s - 0.5 * o for s, o in zip(sum_one, one)])
        turned = coupled(factor, sum_one)
        inner = [begin[k] + moved[k] + turned[k] for k in range(2)]
        node_one = [inside * f for f in times(*inverse, inner)]
        moved = times(real, imag, [s - 0.5 * o for s, o in zip(sum_two, two)])
        turned = coupled(
            factor, [sum_two[k] + 0.5 * (node_one[k] - one[k]) for k in range(2)]
        )
        inner = [node_one[k] + moved[k] + turned[k] for k in range(2)]
        node_two = times(*inverse, inner)
        own = slice(HALO, HALO + BLOCK)
        rows = rows_of(block)
        if not coarse:
            for k in range(2):
                nodes_out[0, k, rows, here] = node_one[k][own]
                nodes_out[1, k, rows, here] = node_two[k][own]
            return
        mean = weighted(whole_weights, (begin, node_one, node_two))
        moved = times(real, imag, [mean[k] - node_two[k] for k in range(2)])
        turned = coupled(factor, mean)
        offset = [moved[k] + turned[k] for k in range(2)]
        step_real, step_imag = 1.0 - real, -imag
        scale = 1.0 / (step_real * step_real + step_imag * step_imag)
        grown = (step_real * scale, -step_imag * scale)
        offset = times(*grown, offset)
        local = pl.ds(pl.multiple_of(block * BLOCK - coarse_start, BLOCK), BLOCK)
        inner_here = pl.ds(pl.multiple_of(column - low_column, LANES), LANES)
        for k in range(2):
            gain[k, local, inner_here] = grown[k][own]
            shift[k, local, inner_here] = offset[k][own]
            kept = node_one[k] - 0.5 * (begin[k] + node_two[k])
            nodes_out[0, k, rows, here] = kept[own]

    lead = jnp.where(first == 0, 2, 3)

    def compute(step, after=None):
        block = block_of(step)
        arrived = jnp.where(step == 0, 0, step + lead - 1)

        @pl.loop(arrived, jnp.minimum(step + lead, blocks))
        def _(which):
            for c in loads(which):
                c.wait()

        @pl.when((block == blocks - 1) & has_down)
        def _():
            for c in halos(0):
                c.wait_recv()

        @pl.when((block == 0) & has_up)
        def _():
            for c in halos(1):
                c.wait_recv()

        in_coarse = coarse_rank & (step < coarse_blocks)
        strips = columns // LANES // PARTS

        @pl.loop(0, PARTS)
        def _(part):
            @pl.loop(0, strips)
            def _(index):
                low = (part * strips + index) * LANES
                column = pl.multiple_of(low, LANES)
                if after is not None:
                    strip_compute(block, column, False)
                    return
                coarse = in_coarse & (low >= low_column) & (low < low_column + CX)

                @pl.when(coarse)
                def _():
                    strip_compute(block, column, True)

                @pl.when(jnp.logical_not(coarse))
                def _():
                    strip_compute(block, column, False)

            if after is not None:
                after(PARTS * step + part)

    def relay():
        @pl.when(jnp.logical_not(has_prev))
        def _():
            whole_start.wait()

        @pl.loop(0, coarse_blocks)
        def _(step):
            @pl.when(has_prev)
            def _():
                relay_copy(step).wait_recv()

            block = block_of(step)
            rows = rows_of(block)
            local = pl.ds(pl.multiple_of(block * BLOCK - coarse_start, BLOCK), BLOCK)
            here = pl.ds(low_column, CX)
            begin = [start_out[k, rows, here] for k in range(2)]
            grown = times(gain[0, local, :], gain[1, local, :], begin)
            finish = [grown[k] + shift[k, local, :] for k in range(2)]
            for k in range(2):
                nodes_out[1, k, rows, here] = finish[k]

            @pl.when(has_next)
            def _():
                relay_copy(step).start()

            for k in range(2):
                nodes_out[0, k, rows, here] += 0.5 * (begin[k] + finish[k])

    units = PARTS * blocks
    waiting = jnp.minimum(PARTS * tm // 2, units)
    opening = jnp.where(has_prev, jnp.minimum(waiting, PARTS * coarse_blocks), PARTS * coarse_blocks)
    middle = jnp.maximum(waiting, opening)

    @pl.when(coarse_rank)
    def _():
        greet()

        @pl.loop(0, coarse_blocks)
        def _(step):
            compute(step)

        @pl.when(jnp.logical_not(has_prev))
        def _():
            relay()

        send(0, opening)

        @pl.loop(coarse_blocks, blocks)
        def _(step):
            compute(step)

        send(opening, middle)

        @pl.when(has_prev)
        def _():
            relay()

        send(middle, units)

    @pl.when(jnp.logical_not(coarse_rank))
    def _():
        def after(unit):
            @pl.when(unit == 0)
            def _():
                greet()

            send(unit, unit + 1)

        @pl.loop(0, blocks)
        def _(step):
            compute(step, after)

        @pl.when(jnp.logical_not(has_prev))
        def _():
            whole_start.wait()

    for side, exists in ((0, has_up), (1, has_down)):

        @pl.when(exists)
        def _(side=side):
            for c in halos(side):
                c.wait_send()

    @pl.when(coarse_rank & has_next)
    def _():
        @pl.loop(0, coarse_blocks)
        def _(step):
            relay_copy(step).wait_send()

    @pl.when(has_prev)
    def _():
        @pl.loop(0, units)
        def _(unit):
            bulk(unit, lambda c: c.wait_recv())

    @pl.when(has_next)
    def _():
        @pl.loop(0, units)
        def _(unit):
            bulk(unit, lambda c: c.wait_send())


def write_out(start, nodes, start_hbm, nodes_hbm, sem):
    copies = [
        pltpu.make_async_copy(nodes.at[f, k], nodes_hbm.at[f, k], sem.at[2 * f + k])
        for f in range(2)
        for k in range(2)
    ]
    copies += [pltpu.make_async_copy(start.at[k], start_hbm.at[k], sem.at[4 + k]) for k in range(2)]
    for c in copies:
        c.start()
    for c in copies:
        c.wait()


def body(start_values, node_values):
    slab, columns = start_values.shape[2:]
    peers = lax.axis_size("space")
    coarse_rows = min(slab, max(CX // 2, CX // peers))
    blocks, coarse_blocks = slab // BLOCK, coarse_rows // BLOCK
    hbm = pl.BlockSpec(memory_space=pltpu.HBM)
    vmem = pl.BlockSpec(memory_space=pltpu.VMEM)
    dma = pltpu.SemaphoreType.DMA
    start, nodes = pl.pallas_call(
        kernel,
        out_shape=(
            OUT((2, slab, columns), jnp.float32),
            OUT((2, 2, slab, columns), jnp.float32),
        ),
        in_specs=[hbm, hbm],
        out_specs=(vmem, vmem),
        scratch_shapes=[
            pltpu.VMEM((3, 2, slab + 2 * HALO, columns), jnp.float32),
            pltpu.VMEM((2, coarse_rows, CX), jnp.float32),
            pltpu.VMEM((2, coarse_rows, CX), jnp.float32),
            dma((2, blocks)),
            dma,
            dma((2, 2)),
            dma((2, 2)),
            dma((PARTS * blocks,)),
            dma((PARTS * blocks,)),
            dma((coarse_blocks,)),
            dma((coarse_blocks,)),
        ],
        compiler_params=pltpu.CompilerParams(
            collective_id=0, has_side_effects=True, vmem_limit_bytes=56 * 1024 * 1024
        ),
    )(start_values[0], node_values[0])
    start, nodes = pl.pallas_call(
        write_out,
        out_shape=(
            jax.ShapeDtypeStruct(start.shape, jnp.float32),
            jax.ShapeDtypeStruct(nodes.shape, jnp.float32),
        ),
        in_specs=[pl.BlockSpec(memory_space=pl.ANY)] * 2,
        out_specs=(hbm, hbm),
        scratch_shapes=[dma((6,))],
        compiler_params=pltpu.CompilerParams(vmem_limit_bytes=2 * 1024 * 1024),
    )(start, nodes)
    return (start[None], nodes[None])


OUT = pltpu.VMEM


def solution(mesh):
    in_specs = (P("tm", None, "space", None), P("tm", None, None, "space", None))
    out_specs = (P("tm", None, "space", None), P("tm", None, None, "space", None))
    return jax.shard_map(body, mesh=mesh, in_specs=in_specs, out_specs=out_specs, check_vma=False)
```
